32 devices in a mesh: group: 4 (over y, x), dev: 8 (over z, core).
Axes of the slice: x: 2, y: 2, z: 4, core: 2. Of those that a mesh axis runs over, the one named last changes fastest.
Arguments:
- fluid_state: float32 [4, 4, 16, 128, 128], P('group', None, None, 'dev'), may hold values from -6 to 6
- coupling: float32 [4, 4], replicated, may hold values from -2.5 to 2.5
- displacement: float32 [3, 32768], P(None, 'dev'), may hold values from -6 to 6
- slot_cells: int32 [4, 8, 8, 8, 128], P('group', 'dev'), may hold values from 0 to 32767
- slot_weights: float32 [4, 8, 8, 8, 128], P('group', 'dev'), may hold values from 0.05 to 0.25
- slot_nodes: int32 [4, 8, 8, 128], P('group', 'dev'), may hold values from 0 to 4095
- slot_counts: int32 [4, 8, 8], P('group', 'dev'), may hold values from 1 to 128, as said below
- flexibility: float32 [24, 24, 4096], P(None, None, 'dev'), may hold values from -1.25 to 1.25
- resid_prev: float32 [3, 32768], P(None, 'dev'), may hold values from -520 to 520
- struct_prev: float32 [3, 32768], P(None, 'dev'), may hold values from -6 to 6
- v_hist: float32 [7, 3, 32768], P(None, None, 'dev'), may hold values from -80 to 80
- w_hist: float32 [7, 3, 32768], P(None, None, 'dev'), may hold values from -6 to 6
Outputs:
- fluid_out: float32 [4, 4, 16, 128, 128], P('group', None, None, 'dev')
- updated: float32 [3, 32768], P(None, 'dev')
The draws below stay inside these ranges and needn't reach their ends.
Inputs may be any that keep to these rules, and one draw needn't show every extreme that they name: `slot_counts`: slots at and beyond the count are padding.
All inputs are finite; a program needn't handle non-finite values.
Results may differ from the reference program's by a relative error of at most 0.0003.
Values sent between devices are 32-bit elements; how exact they have to be, the bound alone decides.
A program may use at most 128 MiB of HBM per device.

```python
import jax
import jax.numpy as jnp
from jax import lax

CX = 16
CY = 128
CZ = 16
IF_DEV = 4096
HIST = 7
CAP = 128
NX = 128
NIF = 32768
N_GROUP = 4
N_DEV = 8


def history_parts(key):
    scale_key = jax.random.fold_in(key, 101)
    column_key = jax.random.fold_in(key, 102)
    mixing_key = jax.random.fold_in(key, 103)
    own_key = jax.random.fold_in(key, 104)
    common_key = jax.random.fold_in(key, 105)
    weight_key = jax.random.fold_in(key, 106)
    scales = jnp.exp(jax.random.uniform(scale_key, (HIST, 1, 1), jnp.float32, 0.0, 1.0986))
    position = jnp.arange(NIF, dtype=jnp.int32).astype(jnp.float32) / NIF
    common_weights = jax.random.uniform(weight_key, (HIST, 1, 1), jnp.float32, 0.5, 1.0)
    columns = jax.random.truncated_normal(column_key, -6.0, 6.0, (HIST, 3, NIF), jnp.float32)
    own_part = jax.random.truncated_normal(own_key, -6.0, 6.0, (3, NIF), jnp.float32)
    common = jax.random.truncated_normal(common_key, -6.0, 6.0, (3, NIF), jnp.float32)
    ramp = 0.6 * jnp.exp(jnp.log(5.0) * position)
    columns = (columns + common_weights * (ramp[None] * common)[None]) * scales
    mixing = 0.5 * jax.random.truncated_normal(mixing_key, -2.0, 2.0, (HIST,), jnp.float32)
    previous = jnp.einsum('h,hcn->cn', mixing, columns) + own_part
    return (columns, previous)


def draw_v_hist(key, part):
    return history_parts(key)[0]


def draw_resid_prev(key, part):
    return history_parts(key)[1]


def draw_slot_counts(key, part):
    counts = jax.random.randint(jax.random.fold_in(key, 201), (N_GROUP, N_DEV, N_DEV), 1, CAP + 1)
    full_owner = jax.random.randint(jax.random.fold_in(key, 202), (), 0, N_DEV)
    owners = jnp.arange(N_DEV, dtype=jnp.int32)[None, None, :]
    return jnp.where(owners == full_owner, CAP, counts).astype(jnp.int32)


def touch_ends(values, stream_key, smallest, top_value):
    place = [jax.random.randint(jax.random.fold_in(stream_key, axis), (), 0, length) for axis, length in enumerate(values.shape)]
    main_axis = values.shape.index(max(values.shape))
    next_to = place[:main_axis] + [(place[main_axis] + 1) % values.shape[main_axis]] + place[main_axis + 1:]
    return values.at[tuple(place)].set(smallest).at[tuple(next_to)].set(top_value)


def levels(stream_key, shape, shards, low, top_value):
    level = 1.0
    for axis_at, shards_of in shards:
        draws = jax.random.uniform(jax.random.fold_in(jax.random.fold_in(stream_key, 6), axis_at), (shards_of,), jnp.float32, low / len(shards), top_value / len(shards))
        level = level * jnp.repeat(jnp.exp(draws), shape[axis_at] // shards_of).reshape((-1,) + (1,) * (len(shape) - 1 - axis_at))
    return level


def gaussian(key, extent, deviation, most, split=(), kind=jnp.bfloat16):
    drawn = jax.random.normal(key, extent, jnp.float32) * deviation
    if len(split) > 0:
        drawn = levels(key, extent, split, -0.22, 0.18) * drawn
    return jnp.clip(drawn, min=-most, max=most).astype(kind)


def setup_inputs(seed: int = 0) -> dict:
    seeds = jax.random.split(jax.random.key(seed), 13)
    fluid_state = gaussian(seeds[0], (N_GROUP, 4, CZ, NX, CY), 1.0, 6.0, ((0, 4), (3, 8)), jnp.float32)
    coupling = gaussian(seeds[1], (4, 4), 0.5, 2.5, (), jnp.float32)
    displacement = gaussian(seeds[2], (3, NIF), 1.0, 6.0, ((1, 8),), jnp.float32)
    slot_cells = touch_ends(jax.random.randint(seeds[3], (N_GROUP, N_DEV, 8, N_DEV, CAP), 0, CZ * CX * CY), jax.random.fold_in(seeds[3], 1), 0, (CZ * CX * CY) - 1).astype(jnp.int32)
    slot_weights = jnp.clip(0.05 + 0.2 * jax.random.uniform(seeds[4], (N_GROUP, N_DEV, 8, N_DEV, CAP), jnp.float32) ** levels(seeds[4], (N_GROUP, N_DEV, 8, N_DEV, CAP), ((0, 4), (1, 8)), -0.2, 0.2), 0.05, 0.25)
    slot_nodes = touch_ends(jax.random.randint(seeds[5], (N_GROUP, N_DEV, N_DEV, CAP), 0, IF_DEV), jax.random.fold_in(seeds[5], 1), 0, IF_DEV - 1).astype(jnp.int32)
    slot_counts = draw_slot_counts(jax.random.fold_in(seeds[12], 71), 0)
    flexibility = gaussian(seeds[7], (24, 24, NIF // 8), 24 ** -0.5, 1.25, ((2, 8),), jnp.float32)
    resid_prev = draw_resid_prev(jax.random.fold_in(seeds[12], 71), 0)
    struct_prev = gaussian(seeds[9], (3, NIF), 1.0, 6.0, ((1, 8),), jnp.float32)
    v_hist = draw_v_hist(jax.random.fold_in(seeds[12], 71), 0)
    w_hist = gaussian(seeds[11], (HIST, 3, NIF), 1.0, 6.0, ((2, 8),), jnp.float32)
    return {"fluid_state": fluid_state, "coupling": coupling, "displacement": displacement, "slot_cells": slot_cells, "slot_weights": slot_weights, "slot_nodes": slot_nodes, "slot_counts": slot_counts, "flexibility": flexibility, "resid_prev": resid_prev, "struct_prev": struct_prev, "v_hist": v_hist, "w_hist": w_hist}


TAU = 0.15
KAPPA = 1.0

def laplace(padded):
    center = padded[:, 1:-1, 1:-1, 1:-1]
    beside = padded[:, 2:, 1:-1, 1:-1] + padded[:, :-2, 1:-1, 1:-1]
    beside = beside + padded[:, 1:-1, 2:, 1:-1] + padded[:, 1:-1, :-2, 1:-1]
    beside = beside + padded[:, 1:-1, 1:-1, 2:] + padded[:, 1:-1, 1:-1, :-2]
    return beside - 6.0 * center

def relax_step(padded_x, forcing, coupling):
    full_pad = jnp.pad(padded_x, ((0, 0), (1, 1), (0, 0), (1, 1)))
    center = padded_x[:, :, 1:-1, :]
    mixing = jnp.einsum('ab,bzxy->azxy', coupling, center, precision=lax.Precision.HIGHEST)
    return center + TAU * (laplace(full_pad) + mixing + forcing)

def comply(flexibility, force_field):
    block_count = force_field.shape[1] // 8
    stacked = force_field.reshape(3, block_count, 8).transpose(0, 2, 1).reshape(24, block_count)
    response = jnp.sum(flexibility * stacked[None], axis=1)
    return response.reshape(3, 8, block_count).transpose(0, 2, 1).reshape(3, block_count * 8)

def to_blocks(field_part):
    comps = field_part.shape[0]
    return field_part.reshape(comps, CZ, N_DEV, CX, CY).transpose(2, 0, 1, 3, 4).reshape(N_DEV, comps, CZ * CX * CY)

def from_blocks(blocks):
    comps = blocks.shape[1]
    return blocks.reshape(N_DEV, comps, CZ, CX, CY).transpose(1, 2, 0, 3, 4).reshape(comps, CZ, N_DEV * CX, CY)

def spread_one(cell_index, weights, arrived):
    contrib = KAPPA * weights[None] * arrived[:, None]
    blank = jnp.zeros((3, CZ * CX * CY), jnp.float32)
    return blank.at[:, cell_index.reshape(-1)].add(contrib.reshape(3, -1))

def sample_one(block, cell_index):
    return block[:, cell_index]

def reference(fluid_state, coupling, displacement, slot_cells, slot_weights, slot_nodes, slot_counts, flexibility, resid_prev, struct_prev, v_hist, w_hist):
    owner_base = jnp.arange(N_DEV, dtype=jnp.int32)[:, None] * IF_DEV
    total_force = jnp.zeros((3, NIF), jnp.float32)
    outputs = []
    for group_id in range(N_GROUP - 1):
        cell_index = slot_cells[group_id]
        weights = slot_weights[group_id]
        global_nodes = (slot_nodes[group_id] + owner_base[None]).astype(jnp.int32)
        live_mask = (jnp.arange(CAP, dtype=jnp.int32)[None, None, :] < slot_counts[group_id][:, :, None]).astype(jnp.float32)
        arrived = displacement[:, global_nodes]
        arrived = jnp.transpose(arrived, (1, 0, 2, 3)) * live_mask[:, None]
        spread = jax.vmap(spread_one)(cell_index, weights, arrived)
        forcing = from_blocks(spread)
        forcing = jnp.concatenate([forcing, jnp.zeros((1, CZ, NX, CY), jnp.float32)])
        current = fluid_state[group_id]
        for sweep_id in range(2):
            current = relax_step(jnp.pad(current, ((0, 0), (0, 0), (1, 1), (0, 0))), forcing, coupling)
        outputs.append(current)
        blocks = to_blocks(current[:3])
        sampled = jax.vmap(sample_one)(blocks, cell_index)
        slot_force = jnp.sum(weights[:, None] * sampled, axis=2) * live_mask[:, None]
        total_force = total_force.at[:, global_nodes].add(jnp.transpose(slot_force, (1, 0, 2, 3)))
    outputs.append(fluid_state[N_GROUP - 1])
    fluid_out = jnp.stack(outputs)
    solid_disp = comply(flexibility, total_force)
    residual = solid_disp - displacement
    basis = jnp.concatenate([(residual - resid_prev)[None], v_hist]).reshape(HIST + 1, -1)
    images = jnp.concatenate([(solid_disp - struct_prev)[None], w_hist]).reshape(HIST + 1, -1)
    gram_matrix = jnp.dot(basis, basis.T, precision=lax.Precision.HIGHEST)
    right_side = jnp.dot(basis, residual.reshape(-1), precision=lax.Precision.HIGHEST)
    factor = jnp.linalg.cholesky(gram_matrix)
    coeffs = -jax.scipy.linalg.cho_solve((factor, True), right_side)
    updated = solid_disp + jnp.dot(coeffs, images, precision=lax.Precision.HIGHEST).reshape(3, -1)
    return (fluid_out, updated)
```

```python
import functools

import jax
import jax.numpy as jnp
from jax import lax
from jax.experimental import pallas as pl
from jax.experimental.pallas import tpu as pltpu
from jax.sharding import PartitionSpec as P

TAU = 0.15
KAPPA = 1.0
MESH = pl.DeviceIdType.MESH
VMEM = pl.BlockSpec(memory_space=pltpu.VMEM)
SMEM = pl.BlockSpec(memory_space=pltpu.SMEM)
F32 = jnp.float32
BF16 = jnp.bfloat16
LANES = 128
ELEM = 8


def log2(n):
    assert n & (n - 1) == 0
    return n.bit_length() - 1


def iota(shape, dim):
    return lax.broadcasted_iota(jnp.int32, shape, dim)


def split(x, terms):
    parts = []
    for _ in range(terms):
        part = x.astype(BF16)
        parts.append(part)
        x = x - part.astype(F32)
    return parts


def hot(rows, index):
    return jnp.where(iota((rows, index.shape[1]), 0) == index, 1.0, 0.0).astype(BF16)


def place():
    return lax.axis_index("group"), lax.axis_index("dev")


def greet(offsets, sizes):
    barrier = pltpu.get_barrier_semaphore()
    me = place()
    for off in offsets:
        target = tuple(lax.rem(m + o, n) for m, o, n in zip(me, off, sizes))
        pl.semaphore_signal(barrier, inc=1, device_id=target, device_id_type=MESH)
    pl.semaphore_wait(barrier, len(offsets))


def all_offsets(sizes):
    return [(a, b) for a in range(sizes[0]) for b in range(sizes[1]) if (a, b) != (0, 0)]


def dev_offsets(sizes):
    return [(0, b) for b in range(1, sizes[1])]


def send(src, dst, send_sem, recv_sem, target):
    return pltpu.make_async_remote_copy(
        src_ref=src, dst_ref=dst, send_sem=send_sem, recv_sem=recv_sem,
        device_id=target, device_id_type=MESH,
    )


def shifted(me, off, sizes):
    return tuple(lax.rem(m + o, n) for m, o, n in zip(me, off, sizes))


def spread_rows(rows_ref, out_ref, sizes, send_sem, recv_sem):
    me = place()
    copies = []
    for off in all_offsets(sizes):
        slot = off[0] * sizes[1] + off[1]
        target = shifted(me, off, sizes)
        copy = send(rows_ref.at[target[1]], out_ref.at[slot], send_sem.at[slot], recv_sem.at[slot], target)
        copy.start()
        copies.append(copy)
    out_ref[0] = rows_ref[me[1]]
    return copies


def halo_copies(edge_ref, halo_ref, sizes, send_sem, recv_sem, act):
    g, s = place()
    count = sizes[1]
    up = send(edge_ref.at[1], halo_ref.at[0], send_sem.at[0], recv_sem.at[0], (g, lax.rem(s + 1, count)))
    down = send(edge_ref.at[0], halo_ref.at[1], send_sem.at[1], recv_sem.at[1], (g, lax.rem(s + count - 1, count)))
    has_up = s < count - 1
    has_down = s > 0
    if act == "start":
        pl.when(has_up)(up.start)
        pl.when(has_down)(down.start)
    else:
        pl.when(has_up)(up.wait_send)
        pl.when(has_down)(down.wait_send)
        pl.when(has_down)(up.wait_recv)
        pl.when(has_up)(down.wait_recv)


def blank_ends(halo_ref, sizes):
    g, s = place()

    @pl.when(s == 0)
    def _():
        halo_ref[0] = jnp.zeros(halo_ref.shape[1:], F32)

    @pl.when(s == sizes[1] - 1)
    def _():
        halo_ref[1] = jnp.zeros(halo_ref.shape[1:], F32)


def index_kernel(sizes, nodes_ref, state_ref, table_ref, halo_ref, rows, edge, ss, rs, hs, hr):
    width = state_ref.shape[3]
    for p in range(sizes[1]):
        rows[p] = nodes_ref[0, 0, p : p + 1, :]
    edge[0] = state_ref[0, :, :, 0:1, :]
    edge[1] = state_ref[0, :, :, width - 1 : width, :]
    greet(all_offsets(sizes), sizes)
    copies = spread_rows(rows, table_ref, sizes, ss, rs)
    halo_copies(edge, halo_ref, sizes, hs, hr, "start")
    blank_ends(halo_ref, sizes)
    for copy in copies:
        copy.wait()
    halo_copies(edge, halo_ref, sizes, hs, hr, "wait")


def pick_kernel(sizes, disp_ref, table_ref, out_ref, flat, picked, ss, rs):
    count = sizes[1]
    highs = disp_ref.shape[1] // LANES
    for c in range(3):
        for h in range(highs):
            flat[c * highs + h : c * highs + h + 1, :] = disp_ref[c : c + 1, h * LANES : (h + 1) * LANES]
    left = jnp.concatenate(split(flat[...], 3), axis=1)
    shift = log2(LANES)
    for b in range(count):
        node = table_ref[b]
        low = hot(LANES, node & (LANES - 1))
        got = jnp.dot(left, jnp.concatenate([low] * 3, axis=0), preferred_element_type=F32)
        mask = iota((highs, LANES), 0) == (node >> shift)
        for c in range(3):
            part = jnp.where(mask, got[c * highs : (c + 1) * highs, :], 0.0)
            picked[b, c : c + 1, :] = jnp.sum(part, axis=0, keepdims=True)
    offsets = dev_offsets(sizes)
    greet(offsets, sizes)
    me = place()
    copies = []
    for off in offsets:
        b = off[1]
        target = shifted(me, (0, count - b), sizes)
        copy = send(picked.at[b], out_ref.at[b], ss.at[b], rs.at[b], target)
        copy.start()
        copies.append(copy)
    out_ref[0] = picked[0]
    for copy in copies:
        copy.wait()


def live_rows(counts_ref, p, capacity):
    g, _ = place()
    top = jnp.where(g < lax.axis_size("group") - 1, counts_ref[0, 0, p], 0)
    return jnp.where(iota((1, capacity), 1) < top, 1.0, 0.0)


def sweep(q_ref, halo_ref, forcing_ref, coupling_ref, out_ref, out_lead, q_lead):
    comps, depth, width, span = q_ref.shape[-4:]

    def body(z, carry):
        lane = iota((width, span), 1)
        sub = iota((width, span), 0)
        low_z = jnp.where(z > 0, 1.0, 0.0)
        high_z = jnp.where(z < depth - 1, 1.0, 0.0)
        centers = [q_ref[(*q_lead, a, z)] for a in range(comps)]
        for a in range(comps):
            c = centers[a]
            near = q_ref[(*q_lead, a, jnp.maximum(z - 1, 0))] * low_z
            near = near + q_ref[(*q_lead, a, jnp.minimum(z + 1, depth - 1))] * high_z
            near = near + jnp.where(sub == 0, halo_ref[0, a, z], pltpu.roll(c, 1, 0))
            near = near + jnp.where(sub == width - 1, halo_ref[1, a, z], pltpu.roll(c, width - 1, 0))
            near = near + jnp.where(lane == 0, 0.0, pltpu.roll(c, 1, 1))
            near = near + jnp.where(lane == span - 1, 0.0, pltpu.roll(c, span - 1, 1))
            mixed = near - 6.0 * c
            for b in range(comps):
                mixed = mixed + coupling_ref[a, b] * centers[b]
            if a < 3:
                mixed = mixed + forcing_ref[z, :, a * span : (a + 1) * span]
            out_ref[(*out_lead, a, z)] = c + TAU * mixed
        return carry

    lax.fori_loop(0, depth, body, 0)


def spread_kernel(
    count, arrived_ref, counts_ref, cells_ref, weights_ref, state_ref, halo_ref, coupling_ref,
    forcing_ref, first_ref, edge_ref, total, masked,
):
    depth, width, span = state_ref.shape[-3:]
    capacity = arrived_ref.shape[2]
    row_count = depth * width
    shift = log2(span)
    _, s = place()
    for p in range(count):
        masked[p] = arrived_ref[lax.rem(p - s + count, count)] * live_rows(counts_ref, p, capacity)
    total[...] = jnp.zeros(total.shape, F32)

    def corner(j, carry):
        cell = cells_ref[0, 0, j]
        weight = weights_ref[0, 0, j]
        left, high, low = [], [], []
        for p in range(count):
            index = cell[p : p + 1, :]
            left.append(hot(row_count, index >> shift))
            mask = iota((span, capacity), 0) == (index & (span - 1))
            scaled = KAPPA * weight[p : p + 1, :] * masked[p]
            parts = split(scaled, 2)
            for into, part in zip((high, low), parts):
                part = part.astype(F32)
                into.append(
                    jnp.concatenate(
                        [jnp.where(mask, part[c : c + 1, :], 0.0).astype(BF16) for c in range(3)], axis=0
                    )
                )
        left = jnp.concatenate(left, axis=1)
        for right in (high, low):
            total[...] += lax.dot_general(
                left, jnp.concatenate(right, axis=1), (((1,), (1,)), ((), ())), preferred_element_type=F32
            )
        return carry

    lax.fori_loop(0, cells_ref.shape[2], corner, 0)
    forcing_ref[...] = total[...].reshape(depth, width, 3 * span)
    sweep(state_ref, halo_ref, forcing_ref, coupling_ref, first_ref, (), (0,))
    edge_ref[0] = first_ref[:, :, 0:1, :]
    edge_ref[1] = first_ref[:, :, width - 1 : width, :]


def halo_kernel(sizes, edge_ref, halo_ref, hs, hr):
    greet([(0, 1), (0, sizes[1] - 1)], sizes)
    halo_copies(edge_ref, halo_ref, sizes, hs, hr, "start")
    blank_ends(halo_ref, sizes)
    halo_copies(edge_ref, halo_ref, sizes, hs, hr, "wait")


def sample_kernel(
    count, first_ref, halo_ref, forcing_ref, coupling_ref, state_ref, cells_ref, weights_ref, counts_ref,
    out_ref, force_ref, table,
):
    depth, width, span = state_ref.shape[-3:]
    capacity = cells_ref.shape[-1]
    row_count = depth * width
    shift = log2(span)
    g, _ = place()
    fluid = g < lax.axis_size("group") - 1
    sweep(first_ref, halo_ref, forcing_ref, coupling_ref, out_ref, (0,), ())
    for c in range(3):
        parts = split(out_ref[0, c].reshape(row_count, span).T, 2)
        for t, part in enumerate(parts):
            table[c * span : (c + 1) * span, t * row_count : (t + 1) * row_count] = part

    @pl.when(jnp.logical_not(fluid))
    def _():
        out_ref[...] = state_ref[...]

    force_ref[...] = jnp.zeros(force_ref.shape, F32)

    def corner(j, carry):
        cell = cells_ref[0, 0, j]
        weight = weights_ref[0, 0, j]
        rows = jnp.concatenate([hot(row_count, cell[p : p + 1, :] >> shift) for p in range(count)], axis=1)
        got = jnp.dot(table[...], jnp.concatenate([rows, rows], axis=0), preferred_element_type=F32)
        for p in range(count):
            mask = iota((span, capacity), 0) == (cell[p : p + 1, :] & (span - 1))
            for c in range(3):
                part = jnp.where(mask, got[c * span : (c + 1) * span, p * capacity : (p + 1) * capacity], 0.0)
                value = jnp.sum(part, axis=0, keepdims=True) * weight[p : p + 1, :]
                force_ref[p, c : c + 1, :] += value
        return carry

    lax.fori_loop(0, cells_ref.shape[2], corner, 0)
    for p in range(count):
        force_ref[p] = force_ref[p] * live_rows(counts_ref, p, capacity)


def force_kernel(sizes, rows_ref, out_ref, ss, rs):
    greet(all_offsets(sizes), sizes)
    for copy in spread_rows(rows_ref, out_ref, sizes, ss, rs):
        copy.wait()


def fold(product):
    total = product[:, :LANES]
    for h in range(1, product.shape[1] // LANES):
        total = total + product[:, h * LANES : (h + 1) * LANES]
    return jnp.sum(total, axis=0, keepdims=True)


def solid_kernel(
    sizes, table_ref, force_ref, flex_ref, disp_ref, prev_ref, hist_ref, solid_ref, gram_ref, total, nodal, partial
):
    groups, count = sizes
    g, _ = place()
    capacity = table_ref.shape[2]
    n_local = disp_ref.shape[1]
    blocks = n_local // ELEM
    wide = blocks // LANES
    elem_shift, lane_shift = log2(ELEM), log2(LANES)
    total[...] = jnp.zeros(total.shape, F32)

    def source_group(gs, carry):
        base = lax.rem(g - gs + groups, groups) * count
        left, high, low = [], [], []
        for b in range(count):
            node = table_ref[base + b]
            block = node >> elem_shift
            row = (block >> lane_shift) * ELEM + (node & (ELEM - 1))
            left.append(hot(wide * ELEM, row))
            mask = iota((LANES, capacity), 0) == (block & (LANES - 1))
            for into, part in zip((high, low), split(force_ref[base + b], 2)):
                part = part.astype(F32)
                into.append(
                    jnp.concatenate(
                        [jnp.where(mask, part[c : c + 1, :], 0.0).astype(BF16) for c in range(3)], axis=0
                    )
                )
        left = jnp.concatenate(left, axis=1)
        for right in (high, low):
            total[...] += lax.dot_general(
                left, jnp.concatenate(right, axis=1), (((1,), (1,)), ((), ())), preferred_element_type=F32
            )
        return carry

    lax.fori_loop(0, groups - 1, source_group, 0)
    u = jnp.concatenate(
        [
            jnp.concatenate(
                [total[h * ELEM : (h + 1) * ELEM, c * LANES : (c + 1) * LANES] for h in range(wide)], axis=1
            )
            for c in range(3)
        ],
        axis=0,
    )
    for o in range(3 * ELEM):
        nodal[o : o + 1, :] = jnp.sum(flex_ref[o] * u, axis=0, keepdims=True)

    per_row = LANES // ELEM
    own = iota((ELEM, LANES), 0) == (iota((ELEM, LANES), 1) >> log2(per_row))
    lines = []
    for c in range(3):
        for h in range(wide):
            lines.append(
                jnp.concatenate(
                    [
                        jnp.where(own, nodal[c * ELEM + i : c * ELEM + i + 1, h * LANES : (h + 1) * LANES], 0.0)
                        for i in range(ELEM)
                    ],
                    axis=1,
                )
            )
    lines = jnp.concatenate(lines, axis=0)
    k = iota((ELEM * LANES, LANES), 0)
    move = (k & (per_row - 1)) * ELEM + (k >> lane_shift)
    move = jnp.where(move == iota((ELEM * LANES, LANES), 1), 1.0, 0.0).astype(BF16)
    solid = 0.0
    for part in reversed(split(lines, 3)):
        solid = solid + jnp.dot(part, move, preferred_element_type=F32)
    per_comp = n_local // LANES
    for c in range(3):
        for h in range(per_comp):
            solid_ref[c : c + 1, h * LANES : (h + 1) * LANES] = solid[c * per_comp + h : c * per_comp + h + 1, :]

    hist = hist_ref.shape[0]
    order = hist + 1
    residual = solid_ref[...] - disp_ref[...]
    change = residual - prev_ref[...]
    rows = [change] + [hist_ref[h] for h in range(hist)]
    for r in range(order):
        for col in range(r, order):
            value = fold(rows[r] * rows[col])
            partial[col, r : r + 1, :] = value
            if col != r:
                partial[r, col : col + 1, :] = value
        partial[order, r : r + 1, :] = fold(rows[r] * residual)
    lane = iota((order, LANES), 1)
    gram = jnp.zeros((order, LANES), F32)
    for col in range(order + 1):
        gram = gram + jnp.where(lane == col, jnp.sum(partial[col], axis=1, keepdims=True), 0.0)
    gram_ref[...] = gram


def update_kernel(sizes, gram_ref, solid_ref, prev_ref, hist_ref, out_ref, parts, ss, rs):
    offsets = dev_offsets(sizes)
    greet(offsets, sizes)
    me = place()
    copies = []
    for off in offsets:
        b = off[1]
        copy = send(gram_ref, parts.at[b], ss.at[b], rs.at[b], shifted(me, off, sizes))
        copy.start()
        copies.append(copy)
    for copy in copies:
        copy.wait()
    order = gram_ref.shape[0]
    m = jnp.zeros(gram_ref.shape, F32)
    parts[0] = gram_ref[...]
    for owner in range(sizes[1]):
        m = m + parts[lax.rem(me[1] - owner + sizes[1], sizes[1])]
    sub = iota(m.shape, 0)
    for k in range(order):
        row = m[k : k + 1, :] / m[k : k + 1, k : k + 1]
        m = jnp.where(sub == k, row, m - m[:, k : k + 1] * row)
    solid = solid_ref[...]
    result = solid - m[0:1, order : order + 1] * (solid - prev_ref[...])
    for h in range(order - 1):
        result = result - m[h + 1 : h + 2, order : order + 1] * hist_ref[h]
    out_ref[...] = result


def call(kernel, outs, ins, scratch=(), collective=None, side=False):
    return pl.pallas_call(
        kernel,
        out_shape=tuple(jax.ShapeDtypeStruct(*o) for o in outs),
        in_specs=list(ins),
        out_specs=tuple(VMEM for _ in outs),
        scratch_shapes=list(scratch),
        compiler_params=pltpu.CompilerParams(
            collective_id=collective, has_side_effects=side, vmem_limit_bytes=48 * 1024 * 1024
        ),
    )


def per_device(
    sizes, fluid_state, coupling, displacement, slot_cells, slot_weights, slot_nodes, slot_counts,
    flexibility, resid_prev, struct_prev, v_hist, w_hist,
):
    groups, count = sizes
    total = groups * count
    comps, depth, width, span = fluid_state.shape[1:]
    capacity = slot_nodes.shape[-1]
    n_local = displacement.shape[1]
    order = v_hist.shape[0] + 1
    dma = pltpu.SemaphoreType.DMA
    halo = (2, comps, depth, 1, span)
    table, halo_zero = call(
        functools.partial(index_kernel, sizes),
        [((total, 1, capacity), jnp.int32), (halo, F32)],
        [VMEM, VMEM],
        [
            pltpu.VMEM((count, 1, capacity), jnp.int32), pltpu.VMEM(halo, F32),
            dma((total,)), dma((total,)), dma((2,)), dma((2,)),
        ],
        0, True,
    )(slot_nodes, fluid_state)
    (arrived,) = call(
        functools.partial(pick_kernel, sizes),
        [((count, 3, capacity), F32)],
        [VMEM, VMEM],
        [
            pltpu.VMEM((3 * n_local // LANES, LANES), F32), pltpu.VMEM((count, 3, capacity), F32),
            dma((count,)), dma((count,)),
        ],
        1, True,
    )(displacement, table)
    forcing, first, edge = call(
        functools.partial(spread_kernel, count),
        [((depth, width, 3 * span), F32), ((comps, depth, width, span), F32), (halo, F32)],
        [VMEM, SMEM, VMEM, VMEM, VMEM, VMEM, SMEM],
        [pltpu.VMEM((depth * width, 3 * span), F32), pltpu.VMEM((count, 3, capacity), F32)],
    )(arrived, slot_counts, slot_cells, slot_weights, fluid_state, halo_zero, coupling)
    (halo_one,) = call(
        functools.partial(halo_kernel, sizes), [(halo, F32)], [VMEM], [dma((2,)), dma((2,))], 2, True
    )(edge)
    fluid_out, force = call(
        functools.partial(sample_kernel, count),
        [(fluid_state.shape, F32), ((count, 3, capacity), F32)],
        [VMEM, VMEM, VMEM, SMEM, VMEM, VMEM, VMEM, SMEM],
        [pltpu.VMEM((3 * span, 2 * depth * width), BF16)],
    )(first, halo_one, forcing, coupling, fluid_state, slot_cells, slot_weights, slot_counts)
    (forces,) = call(
        functools.partial(force_kernel, sizes),
        [((total, 3, capacity), F32)], [VMEM], [dma((total,)), dma((total,))], 3, True,
    )(force)
    solid, gram = call(
        functools.partial(solid_kernel, sizes),
        [((3, n_local), F32), ((order, LANES), F32)],
        [VMEM] * 6,
        [
            pltpu.VMEM((n_local // LANES, 3 * LANES), F32), pltpu.VMEM((3 * ELEM, n_local // ELEM), F32),
            pltpu.VMEM((order + 1, order, LANES), F32),
        ],
    )(table, forces, flexibility, displacement, resid_prev, v_hist)
    (updated,) = call(
        functools.partial(update_kernel, sizes),
        [((3, n_local), F32)],
        [VMEM] * 4,
        [pltpu.VMEM((count, order, LANES), F32), dma((count,)), dma((count,))],
        4, True,
    )(gram, solid, struct_prev, w_hist)
    return fluid_out, updated


def solution(mesh):
    sizes = (mesh.shape["group"], mesh.shape["dev"])
    return jax.shard_map(
        functools.partial(per_device, sizes),
        mesh=mesh,
        in_specs=(
            P("group", None, None, "dev", None),
            P(),
            P(None, "dev"),
            P("group", "dev", None, None, None),
            P("group", "dev", None, None, None),
            P("group", "dev", None, None),
            P("group", "dev", None),
            P(None, None, "dev"),
            P(None, "dev"),
            P(None, "dev"),
            P(None, None, "dev"),
            P(None, None, "dev"),
        ),
        out_specs=(P("group", None, None, "dev", None), P(None, "dev")),
        check_vma=False,
    )
```

```python
import functools

import jax
import jax.numpy as jnp
from jax import lax
from jax.experimental import pallas as pl
from jax.experimental.pallas import tpu as pltpu
from jax.sharding import PartitionSpec as P

TAU = 0.15
KAPPA = 1.0
MESH = pl.DeviceIdType.MESH
F32 = jnp.float32
BF16 = jnp.bfloat16
LANES = 128
ELEM = 8


def log2(n):
    assert n & (n - 1) == 0
    return n.bit_length() - 1


def iota(shape, dim):
    return lax.broadcasted_iota(jnp.int32, shape, dim)


def split(x, terms):
    parts = []
    for _ in range(terms):
        part = x.astype(BF16)
        parts.append(part)
        x = x - part.astype(F32)
    return parts


def hot(rows, index):
    return jnp.where(iota((rows, index.shape[1]), 0) == index, 1.0, 0.0).astype(BF16)


def place():
    return lax.axis_index("group"), lax.axis_index("dev")


def greet(offsets, sizes):
    barrier = pltpu.get_barrier_semaphore()
    me = place()
    for off in offsets:
        target = tuple(lax.rem(m + o, n) for m, o, n in zip(me, off, sizes))
        pl.semaphore_signal(barrier, inc=1, device_id=target, device_id_type=MESH)
    pl.semaphore_wait(barrier, len(offsets))


def send(src, dst, send_sem, recv_sem, target):
    return pltpu.make_async_remote_copy(
        src_ref=src, dst_ref=dst, send_sem=send_sem, recv_sem=recv_sem,
        device_id=target, device_id_type=MESH,
    )


def shifted(me, off, sizes):
    return tuple(lax.rem(m + o, n) for m, o, n in zip(me, off, sizes))


def halo_copies(edge_ref, halo_ref, sizes, send_sem, recv_sem, act):
    g, s = place()
    count = sizes[1]
    up = send(edge_ref.at[1], halo_ref.at[0], send_sem.at[0], recv_sem.at[0], (g, lax.rem(s + 1, count)))
    down = send(edge_ref.at[0], halo_ref.at[1], send_sem.at[1], recv_sem.at[1], (g, lax.rem(s + count - 1, count)))
    has_up = s < count - 1
    has_down = s > 0
    if act == "start":
        pl.when(has_up)(up.start)
        pl.when(has_down)(down.start)
    else:
        pl.when(has_up)(up.wait_send)
        pl.when(has_down)(down.wait_send)
        pl.when(has_down)(up.wait_recv)
        pl.when(has_up)(down.wait_recv)


def blank_ends(halo_ref, sizes):
    g, s = place()

    @pl.when(s == 0)
    def _():
        halo_ref[0] = jnp.zeros(halo_ref.shape[1:], F32)

    @pl.when(s == sizes[1] - 1)
    def _():
        halo_ref[1] = jnp.zeros(halo_ref.shape[1:], F32)


def live_rows(counts_ref, p, capacity):
    g, _ = place()
    top = jnp.where(g < lax.axis_size("group") - 1, counts_ref[0, 0, p], 0)
    return jnp.where(iota((1, capacity), 1) < top, 1.0, 0.0)


def sweep(q_ref, q_lead, forcing_ref, coupling_ref, out_ref):
    comps, depth, width, span = q_ref.shape[-4:]

    def body(z, carry):
        lane = iota((width, span), 1)
        sub = iota((width, span), 0)
        low_z = jnp.where(z > 0, 1.0, 0.0)
        high_z = jnp.where(z < depth - 1, 1.0, 0.0)
        centers = [q_ref[(*q_lead, a, z)] for a in range(comps)]
        for a in range(comps):
            c = centers[a]
            near = q_ref[(*q_lead, a, jnp.maximum(z - 1, 0))] * low_z
            near = near + q_ref[(*q_lead, a, jnp.minimum(z + 1, depth - 1))] * high_z
            near = near + jnp.where(sub == 0, 0.0, pltpu.roll(c, 1, 0))
            near = near + jnp.where(sub == width - 1, 0.0, pltpu.roll(c, width - 1, 0))
            near = near + jnp.where(lane == 0, 0.0, pltpu.roll(c, 1, 1))
            near = near + jnp.where(lane == span - 1, 0.0, pltpu.roll(c, span - 1, 1))
            mixed = near - 6.0 * c
            for b in range(comps):
                mixed = mixed + coupling_ref[a, b] * centers[b]
            if a < 3 and forcing_ref is not None:
                mixed = mixed + forcing_ref[pl.ds(pl.multiple_of(z * width, width), width), a * span : (a + 1) * span]
            out_ref[a, z] = c + TAU * mixed
        return carry

    lax.fori_loop(0, depth, body, 0)


def add_halo(field_ref, halo_ref):
    width = field_ref.shape[2]
    field_ref[:, :, 0:1, :] += TAU * halo_ref[0]
    field_ref[:, :, width - 1 : width, :] += TAU * halo_ref[1]


def take_edges(field_ref, lead, edge_ref):
    width = field_ref.shape[-2]
    edge_ref[0] = field_ref[(*lead, slice(None), slice(None), slice(0, 1), slice(None))]
    edge_ref[1] = field_ref[(*lead, slice(None), slice(None), slice(width - 1, width), slice(None))]


def spread_right(mask, values):
    values = values.astype(F32)
    return jnp.concatenate([jnp.where(mask, values[c : c + 1, :], 0.0).astype(BF16) for c in range(3)], axis=0)


def nt(left, right):
    return lax.dot_general(left, right, (((1,), (1,)), ((), ())), preferred_element_type=F32)


def kernel(
    sizes,
    state_h, coupling_h, disp_h, cells_h, weights_h, nodes_h, counts_h, flex_h, rprev_h, sprev_h, vhist_h, whist_h,
    fluid_h, updated_h,
    state, coupling, disp, cells, weights, nodes, counts, flex, rprev, sprev, vhist, whist,
    in_sems, out_sems, dev_send, dev_recv, group_send, group_recv, halo_send, halo_recv,
    rows, table, edges, halos, flat, picked, arrived, masked, forcing, first, second, sampler,
    force, forces, sums, nodal, solid_s, grams, result,
):
    groups, count = sizes
    me = place()
    g, s = me
    depth, width, span = state.shape[-3:]
    capacity = nodes.shape[-1]
    row_count = depth * width
    n_local = disp.shape[1]
    highs = n_local // LANES
    span_shift, lane_shift, elem_shift = log2(span), log2(LANES), log2(ELEM)

    sources = (nodes_h, state_h, disp_h, coupling_h, counts_h, vhist_h, cells_h, weights_h, flex_h, rprev_h, sprev_h, whist_h)
    targets = (nodes, state, disp, coupling, counts, vhist, cells, weights, flex, rprev, sprev, whist)
    loads = [pltpu.make_async_copy(a, b, in_sems.at[k]) for k, (a, b) in enumerate(zip(sources, targets))]
    for load in loads:
        load.start()
    (l_nodes, l_state, l_disp, l_coupling, l_counts, l_vhist, l_cells, l_weights, l_flex, l_rprev, l_sprev, l_whist) = loads

    l_nodes.wait()
    for p in range(count):
        rows[p] = nodes[0, 0, p : p + 1, :]
    greet([(0, b) for b in range(1, count)] + [(a, 0) for a in range(1, groups)], sizes)

    def to_dev(step, src, dst, b, slot):
        return send(src, dst.at[slot], dev_send.at[step, slot], dev_recv.at[step, slot], shifted(me, (0, b), sizes))

    asked = [to_dev(0, rows.at[lax.rem(s + b, count)], table, b, b) for b in range(1, count)]
    for copy in asked:
        copy.start()
    table[0] = rows[s]

    l_state.wait()
    take_edges(state, (0,), edges.at[0])
    halo_copies(edges.at[0], halos.at[0], sizes, halo_send.at[0], halo_recv.at[0], "start")
    blank_ends(halos.at[0], sizes)

    l_disp.wait()
    for c in range(3):
        for h in range(highs):
            flat[c * highs + h : c * highs + h + 1, :] = disp[c : c + 1, h * LANES : (h + 1) * LANES]
    left = jnp.concatenate(split(flat[...], 3), axis=1)
    answers = []
    for b in range(count):
        if b > 0:
            asked[b - 1].wait_recv()
        node = table[b]
        low = hot(LANES, node & (LANES - 1))
        got = jnp.dot(left, jnp.concatenate([low] * 3, axis=0), preferred_element_type=F32)
        mask = iota((highs, capacity), 0) == (node >> lane_shift)
        for c in range(3):
            part = jnp.where(mask, got[c * highs : (c + 1) * highs, :], 0.0)
            picked[b, c : c + 1, :] = jnp.sum(part, axis=0, keepdims=True)
        if b > 0:
            copy = to_dev(1, picked.at[b], arrived, count - b, b)
            copy.start()
            answers.append(copy)
    arrived[0] = picked[0]

    l_coupling.wait()
    l_counts.wait()
    sweep(state, (0,), None, coupling, first)
    halo_copies(edges.at[0], halos.at[0], sizes, halo_send.at[0], halo_recv.at[0], "wait")
    add_halo(first, halos.at[0])

    l_cells.wait()
    l_weights.wait()
    for copy in answers:
        copy.wait_recv()
    for p in range(count):
        masked[p] = arrived[lax.rem(p - s + count, count)] * live_rows(counts, p, capacity)
    forcing[...] = jnp.zeros(forcing.shape, F32)

    def spread_corner(j, carry):
        cell = cells[0, 0, j]
        weight = weights[0, 0, j]
        left, high, low = [], [], []
        for p in range(count):
            index = cell[p : p + 1, :]
            left.append(hot(row_count, index >> span_shift))
            mask = iota((span, capacity), 0) == (index & (span - 1))
            for into, part in zip((high, low), split(KAPPA * weight[p : p + 1, :] * masked[p], 2)):
                into.append(spread_right(mask, part))
        left = jnp.concatenate(left, axis=1)
        both = nt(left, jnp.concatenate(high, axis=1)) + nt(left, jnp.concatenate(low, axis=1))
        forcing[...] += both
        return carry

    lax.fori_loop(0, cells.shape[2], spread_corner, 0)
    for c in range(3):
        first[c] += TAU * forcing[:, c * span : (c + 1) * span].reshape(depth, width, span)
    take_edges(first, (), edges.at[1])
    halo_copies(edges.at[1], halos.at[1], sizes, halo_send.at[1], halo_recv.at[1], "start")
    blank_ends(halos.at[1], sizes)
    sweep(first, (), forcing, coupling, second)

    l_vhist.wait()
    hist = vhist.shape[1]
    lane = iota((hist, LANES), 1)
    early = jnp.zeros((hist, LANES), F32)
    for h in range(hist):
        product = vhist[0] * vhist[0, h : h + 1, :]
        for c in range(1, 3):
            product = product + vhist[c] * vhist[c, h : h + 1, :]
        early = early + jnp.where(lane == h, jnp.sum(product, axis=1, keepdims=True), 0.0)

    halo_copies(edges.at[1], halos.at[1], sizes, halo_send.at[1], halo_recv.at[1], "wait")
    add_halo(second, halos.at[1])
    fluid = g < groups - 1
    store_fluid = pltpu.make_async_copy(second, fluid_h.at[0], out_sems.at[0])
    store_state = pltpu.make_async_copy(state.at[0], fluid_h.at[0], out_sems.at[0])
    pl.when(fluid)(store_fluid.start)
    pl.when(jnp.logical_not(fluid))(store_state.start)

    for c in range(3):
        for t, part in enumerate(split(second[c].reshape(row_count, span).T, 2)):
            sampler[c * span : (c + 1) * span, t * row_count : (t + 1) * row_count] = part
    force[...] = jnp.zeros(force.shape, F32)

    def sample_corner(j, carry):
        cell = cells[0, 0, j]
        weight = weights[0, 0, j]
        here = jnp.concatenate([hot(row_count, cell[p : p + 1, :] >> span_shift) for p in range(count)], axis=1)
        got = jnp.dot(sampler[...], jnp.concatenate([here, here], axis=0), preferred_element_type=F32)
        for p in range(count):
            mask = iota((span, capacity), 0) == (cell[p : p + 1, :] & (span - 1))
            for c in range(3):
                part = jnp.where(mask, got[c * span : (c + 1) * span, p * capacity : (p + 1) * capacity], 0.0)
                value = jnp.sum(part, axis=0, keepdims=True) * weight[p : p + 1, :]
                force[p, c : c + 1, :] += value
        return carry

    lax.fori_loop(0, cells.shape[2], sample_corner, 0)
    for p in range(count):
        force[p] = force[p] * live_rows(counts, p, capacity)
    pushed = [to_dev(2, force.at[lax.rem(s + b, count)], forces, b, b) for b in range(1, count)]
    for copy in pushed:
        copy.start()
    forces[0] = force[s]

    wide = n_local // ELEM // LANES
    for copy in pushed:
        copy.wait_recv()
    left, high, low = [], [], []
    for b in range(count):
        node = table[b]
        block = node >> elem_shift
        left.append(hot(wide * ELEM, (block >> lane_shift) * ELEM + (node & (ELEM - 1))))
        mask = iota((LANES, capacity), 0) == (block & (LANES - 1))
        for into, part in zip((high, low), split(forces[b], 2)):
            into.append(spread_right(mask, part))
    left = jnp.concatenate(left, axis=1)
    sums[0] = nt(left, jnp.concatenate(high, axis=1)) + nt(left, jnp.concatenate(low, axis=1))
    shared = [
        send(sums.at[0], sums.at[a], group_send.at[a], group_recv.at[a], shifted(me, (a, 0), sizes))
        for a in range(1, groups)
    ]
    for copy in shared:
        copy.start()
    l_flex.wait()
    l_rprev.wait()
    l_sprev.wait()
    l_whist.wait()
    for copy in shared:
        copy.wait_recv()
    total = sums[lax.rem(g + groups, groups)]
    for gs in range(1, groups):
        total = total + sums[lax.rem(g - gs + groups, groups)]
    u = jnp.concatenate(
        [
            jnp.concatenate(
                [total[h * ELEM : (h + 1) * ELEM, c * LANES : (c + 1) * LANES] for h in range(wide)], axis=1
            )
            for c in range(3)
        ],
        axis=0,
    )
    for o in range(3 * ELEM):
        nodal[o : o + 1, :] = jnp.sum(flex[o] * u, axis=0, keepdims=True)

    per_row = LANES // ELEM
    own = iota((ELEM, LANES), 0) == (iota((ELEM, LANES), 1) >> log2(per_row))
    lines = []
    for c in range(3):
        for h in range(wide):
            lines.append(
                jnp.concatenate(
                    [
                        jnp.where(own, nodal[c * ELEM + i : c * ELEM + i + 1, h * LANES : (h + 1) * LANES], 0.0)
                        for i in range(ELEM)
                    ],
                    axis=1,
                )
            )
    lines = jnp.concatenate(lines, axis=0)
    k = iota((ELEM * LANES, LANES), 0)
    move = (k & (per_row - 1)) * ELEM + (k >> lane_shift)
    move = jnp.where(move == iota((ELEM * LANES, LANES), 1), 1.0, 0.0).astype(BF16)
    spread = 0.0
    for part in reversed(split(lines, 3)):
        spread = spread + jnp.dot(part, move, preferred_element_type=F32)
    for c in range(3):
        for h in range(highs):
            solid_s[c : c + 1, h * LANES : (h + 1) * LANES] = spread[c * highs + h : c * highs + h + 1, :]

    order = hist + 1
    solid = solid_s[...]
    residual = solid - disp[...]
    change = residual - rprev[...]
    with_change = vhist[0] * change[0:1, :]
    with_residual = vhist[0] * residual[0:1, :]
    for c in range(1, 3):
        with_change = with_change + vhist[c] * change[c : c + 1, :]
        with_residual = with_residual + vhist[c] * residual[c : c + 1, :]
    cross = jnp.sum(with_change, axis=1, keepdims=True)
    early = early + jnp.where(lane == hist, cross, 0.0)
    early = early + jnp.where(lane == order, jnp.sum(with_residual, axis=1, keepdims=True), 0.0)
    last = jnp.sum(jnp.where(lane == iota((hist, LANES), 0), cross, 0.0), axis=0, keepdims=True)
    lane_one = iota((1, LANES), 1)
    own_square = jnp.sum(jnp.sum(change * change, axis=0, keepdims=True), axis=1, keepdims=True)
    own_right = jnp.sum(jnp.sum(change * residual, axis=0, keepdims=True), axis=1, keepdims=True)
    last = last + jnp.where(lane_one == hist, own_square, 0.0) + jnp.where(lane_one == order, own_right, 0.0)
    grams[0, 0:hist, :] = early
    grams[0, hist : hist + 1, :] = last
    shares = [to_dev(3, grams.at[0], grams, b, b) for b in range(1, count)]
    for copy in shares:
        copy.start()
    image = solid - sprev[...]
    for copy in shares:
        copy.wait_recv()
    m = jnp.zeros((order, LANES), F32)
    for owner in range(count):
        m = m + grams[lax.rem(s - owner + count, count)]
    sub = iota(m.shape, 0)
    for k in range(order):
        row = m[k : k + 1, :] / m[k : k + 1, k : k + 1]
        m = jnp.where(sub == k, row, m - m[:, k : k + 1] * row)
    answer = m[:, order : order + 1]
    for c in range(3):
        old = jnp.sum(answer[0:hist, :] * whist[c], axis=0, keepdims=True)
        result[c : c + 1, :] = solid[c : c + 1, :] - answer[hist : hist + 1, :] * image[c : c + 1, :] - old
    store_result = pltpu.make_async_copy(result, updated_h, out_sems.at[1])
    store_result.start()
    for copy in asked + answers + pushed + shared + shares:
        copy.wait_send()
    pl.when(fluid)(store_fluid.wait)
    pl.when(jnp.logical_not(fluid))(store_state.wait)
    store_result.wait()


def per_device(
    sizes, fluid_state, coupling, displacement, slot_cells, slot_weights, slot_nodes, slot_counts,
    flexibility, resid_prev, struct_prev, v_hist, w_hist,
):
    groups, count = sizes
    comps, depth, width, span = fluid_state.shape[1:]
    capacity = slot_nodes.shape[-1]
    n_local = displacement.shape[1]
    order = v_hist.shape[0] + 1
    dma = pltpu.SemaphoreType.DMA
    vmem = pltpu.VMEM
    args = (
        fluid_state, coupling, displacement, slot_cells, slot_weights, slot_nodes, slot_counts, flexibility,
        resid_prev, struct_prev, v_hist.transpose(1, 0, 2), w_hist.transpose(1, 0, 2),
    )
    small = (1, 6)
    places = [(pltpu.SMEM if k in small else vmem)(a.shape, a.dtype) for k, a in enumerate(args)]
    hbm = pl.BlockSpec(memory_space=pltpu.HBM)
    halo = (2, 2, comps, depth, 1, span)
    slots = (count, 3, capacity)
    return pl.pallas_call(
        functools.partial(kernel, sizes),
        out_shape=(
            jax.ShapeDtypeStruct(fluid_state.shape, F32), jax.ShapeDtypeStruct(displacement.shape, F32),
        ),
        in_specs=[hbm] * len(args),
        out_specs=(hbm, hbm),
        scratch_shapes=places
        + [
            dma((len(args),)), dma((2,)), dma((4, count)), dma((4, count)), dma((groups,)), dma((groups,)),
            dma((2, 2)), dma((2, 2)),
            vmem((count, 1, capacity), jnp.int32), vmem((count, 1, capacity), jnp.int32),
            vmem(halo, F32), vmem(halo, F32),
            vmem((3 * n_local // LANES, LANES), F32), vmem(slots, F32), vmem(slots, F32), vmem(slots, F32),
            vmem((depth * width, 3 * span), F32),
            vmem((comps, depth, width, span), F32), vmem((comps, depth, width, span), F32),
            vmem((3 * span, 2 * depth * width), BF16),
            vmem(slots, F32), vmem(slots, F32), vmem((groups, n_local // LANES, 3 * LANES), F32),
            vmem((3 * ELEM, n_local // ELEM), F32), vmem((3, n_local), F32), vmem((count, order, LANES), F32),
            vmem((3, n_local), F32),
        ],
        compiler_params=pltpu.CompilerParams(
            collective_id=0, has_side_effects=True, vmem_limit_bytes=60 * 1024 * 1024
        ),
    )(*args)


def solution(mesh):
    sizes = (mesh.shape["group"], mesh.shape["dev"])
    return jax.shard_map(
        functools.partial(per_device, sizes),
        mesh=mesh,
        in_specs=(
            P("group", None, None, "dev", None),
            P(),
            P(None, "dev"),
            P("group", "dev", None, None, None),
            P("group", "dev", None, None, None),
            P("group", "dev", None, None),
            P("group", "dev", None),
            P(None, None, "dev"),
            P(None, "dev"),
            P(None, "dev"),
            P(None, None, "dev"),
            P(None, None, "dev"),
        ),
        out_specs=(P("group", None, None, "dev", None), P(None, "dev")),
        check_vma=False,
    )
```

```python
import functools

import jax
import jax.numpy as jnp
from jax import lax
from jax.experimental import pallas as pl
from jax.experimental.pallas import tpu as pltpu
from jax.sharding import PartitionSpec as P

TAU = 0.15
KAPPA = 1.0
MESH = pl.DeviceIdType.MESH
F32 = jnp.float32
BF16 = jnp.bfloat16
LANES = 128
ELEM = 8


def log2(n):
    assert n & (n - 1) == 0
    return n.bit_length() - 1


def iota(shape, dim):
    return lax.broadcasted_iota(jnp.int32, shape, dim)


def split(x, terms):
    parts = []
    for _ in range(terms):
        part = x.astype(BF16)
        parts.append(part)
        x = x - part.astype(F32)
    return parts


def hot(rows, index):
    return jnp.where(iota((rows, index.shape[1]), 0) == index, 1.0, 0.0).astype(BF16)


def place():
    return lax.axis_index("group"), lax.axis_index("dev")


def greet(offsets, sizes):
    barrier = pltpu.get_barrier_semaphore()
    me = place()
    for off in offsets:
        target = tuple(lax.rem(m + o, n) for m, o, n in zip(me, off, sizes))
        pl.semaphore_signal(barrier, inc=1, device_id=target, device_id_type=MESH)
    pl.semaphore_wait(barrier, len(offsets))


def send(src, dst, send_sem, recv_sem, target):
    return pltpu.make_async_remote_copy(
        src_ref=src, dst_ref=dst, send_sem=send_sem, recv_sem=recv_sem,
        device_id=target, device_id_type=MESH,
    )


def shifted(me, off, sizes):
    return tuple(lax.rem(m + o, n) for m, o, n in zip(me, off, sizes))


def halo_copies(edge_ref, halo_ref, sizes, send_sem, recv_sem, act):
    g, s = place()
    count = sizes[1]
    up = send(edge_ref.at[1], halo_ref.at[0], send_sem.at[0], recv_sem.at[0], (g, lax.rem(s + 1, count)))
    down = send(edge_ref.at[0], halo_ref.at[1], send_sem.at[1], recv_sem.at[1], (g, lax.rem(s + count - 1, count)))
    has_up = s < count - 1
    has_down = s > 0
    if act == "start":
        pl.when(has_up)(up.start)
        pl.when(has_down)(down.start)
    else:
        pl.when(has_up)(up.wait_send)
        pl.when(has_down)(down.wait_send)
        pl.when(has_down)(up.wait_recv)
        pl.when(has_up)(down.wait_recv)


def blank_ends(halo_ref, sizes):
    g, s = place()

    @pl.when(s == 0)
    def _():
        halo_ref[0] = jnp.zeros(halo_ref.shape[1:], F32)

    @pl.when(s == sizes[1] - 1)
    def _():
        halo_ref[1] = jnp.zeros(halo_ref.shape[1:], F32)


def live_rows(counts_ref, p, capacity):
    g, _ = place()
    top = jnp.where(g < lax.axis_size("group") - 1, counts_ref[0, 0, p], 0)
    return jnp.where(iota((1, capacity), 1) < top, 1.0, 0.0)


def sweep(q_ref, q_lead, forcing_ref, coupling_ref, out_ref):
    comps, depth, width, span = q_ref.shape[-4:]

    def body(z, carry):
        lane = iota((width, span), 1)
        sub = iota((width, span), 0)
        low_z = jnp.where(z > 0, 1.0, 0.0)
        high_z = jnp.where(z < depth - 1, 1.0, 0.0)
        centers = [q_ref[(*q_lead, a, z)] for a in range(comps)]
        for a in range(comps):
            c = centers[a]
            near = q_ref[(*q_lead, a, jnp.maximum(z - 1, 0))] * low_z
            near = near + q_ref[(*q_lead, a, jnp.minimum(z + 1, depth - 1))] * high_z
            near = near + jnp.where(sub == 0, 0.0, pltpu.roll(c, 1, 0))
            near = near + jnp.where(sub == width - 1, 0.0, pltpu.roll(c, width - 1, 0))
            near = near + jnp.where(lane == 0, 0.0, pltpu.roll(c, 1, 1))
            near = near + jnp.where(lane == span - 1, 0.0, pltpu.roll(c, span - 1, 1))
            mixed = near - 6.0 * c
            for b in range(comps):
                mixed = mixed + coupling_ref[a, b] * centers[b]
            if a < 3 and forcing_ref is not None:
                mixed = mixed + forcing_ref[pl.ds(pl.multiple_of(z * width, width), width), a * span : (a + 1) * span]
            out_ref[a, z] = c + TAU * mixed
        return carry

    lax.fori_loop(0, depth, body, 0)


def add_halo(field_ref, halo_ref):
    width = field_ref.shape[2]
    field_ref[:, :, 0:1, :] += TAU * halo_ref[0]
    field_ref[:, :, width - 1 : width, :] += TAU * halo_ref[1]


def take_edges(field_ref, lead, edge_ref):
    width = field_ref.shape[-2]
    edge_ref[0] = field_ref[(*lead, slice(None), slice(None), slice(0, 1), slice(None))]
    edge_ref[1] = field_ref[(*lead, slice(None), slice(None), slice(width - 1, width), slice(None))]


def spread_right(mask, values):
    values = values.astype(F32)
    return jnp.concatenate([jnp.where(mask, values[c : c + 1, :], 0.0).astype(BF16) for c in range(3)], axis=0)


def scaled_columns(columns, values):
    span, capacity = columns.shape
    tile = 16
    tiles = columns.reshape(span // tile, tile, capacity)
    values = values.astype(F32)
    out = []
    for c in range(3):
        row = jnp.broadcast_to(values[c : c + 1, :], (tile, capacity)).astype(BF16)
        out.append((tiles * row[None]).reshape(span, capacity))
    return jnp.concatenate(out, axis=0)


def nt(left, right):
    return lax.dot_general(left, right, (((1,), (1,)), ((), ())), preferred_element_type=F32)


def kernel(
    sizes,
    state_h, coupling_h, disp_h, cells_h, weights_h, nodes_h, counts_h, flex_h, rprev_h, sprev_h, vhist_h, whist_h,
    fluid_o, result,
    state, coupling, disp, cells, weights, nodes, counts, flex, rprev, sprev, vhist, whist,
    in_sems, dev_send, dev_recv, group_send, group_recv, halo_send, halo_recv,
    rows, table, edges, halos, flat, picked, arrived, masked, forcing, first, second, sampler, row_hot, col_hot,
    force, forces, sums, nodal, solid_s, grams,
):
    groups, count = sizes
    me = place()
    g, s = me
    depth, width, span = state.shape[-3:]
    capacity = nodes.shape[-1]
    row_count = depth * width
    n_local = disp.shape[1]
    highs = n_local // LANES
    span_shift, lane_shift, elem_shift = log2(span), log2(LANES), log2(ELEM)

    sources = (nodes_h, state_h, disp_h, coupling_h, counts_h, vhist_h, cells_h, weights_h, flex_h, rprev_h, sprev_h, whist_h)
    targets = (nodes, state, disp, coupling, counts, vhist, cells, weights, flex, rprev, sprev, whist)
    loads = [pltpu.make_async_copy(a, b, in_sems.at[k]) for k, (a, b) in enumerate(zip(sources, targets))]
    for load in loads:
        load.start()
    (l_nodes, l_state, l_disp, l_coupling, l_counts, l_vhist, l_cells, l_weights, l_flex, l_rprev, l_sprev, l_whist) = loads

    l_nodes.wait()
    for p in range(count):
        rows[p] = nodes[0, 0, p : p + 1, :]
    greet([(0, b) for b in range(1, count)] + [(a, 0) for a in range(1, groups)], sizes)

    def to_dev(step, src, dst, b, slot):
        return send(src, dst.at[slot], dev_send.at[step, slot], dev_recv.at[step, slot], shifted(me, (0, b), sizes))

    asked = [to_dev(0, rows.at[lax.rem(s + b, count)], table, b, b) for b in range(1, count)]
    for copy in asked:
        copy.start()
    table[0] = rows[s]

    l_state.wait()
    take_edges(state, (0,), edges.at[0])
    halo_copies(edges.at[0], halos.at[0], sizes, halo_send.at[0], halo_recv.at[0], "start")
    blank_ends(halos.at[0], sizes)

    l_cells.wait()

    def hot_corner(j, carry):
        cell = cells[0, 0, j]
        for p in range(count):
            at = slice(p * capacity, (p + 1) * capacity)
            row_hot[j, :, at] = hot(row_count, cell[p : p + 1, :] >> span_shift)
            col_hot[j, :, at] = hot(span, cell[p : p + 1, :] & (span - 1))
        return carry

    lax.fori_loop(0, cells.shape[2], hot_corner, 0)

    l_disp.wait()
    for c in range(3):
        for h in range(highs):
            flat[c * highs + h : c * highs + h + 1, :] = disp[c : c + 1, h * LANES : (h + 1) * LANES]
    left = jnp.concatenate(split(flat[...], 3), axis=1)
    answers = []
    for b in range(count):
        if b > 0:
            asked[b - 1].wait_recv()
        node = table[b]
        low = hot(LANES, node & (LANES - 1))
        got = jnp.dot(left, jnp.concatenate([low] * 3, axis=0), preferred_element_type=F32)
        mask = iota((highs, capacity), 0) == (node >> lane_shift)
        for c in range(3):
            part = jnp.where(mask, got[c * highs : (c + 1) * highs, :], 0.0)
            picked[b, c : c + 1, :] = jnp.sum(part, axis=0, keepdims=True)
        if b > 0:
            copy = to_dev(1, picked.at[b], arrived, count - b, b)
            copy.start()
            answers.append(copy)
    arrived[0] = picked[0]

    l_coupling.wait()
    l_counts.wait()
    sweep(state, (0,), None, coupling, first)
    halo_copies(edges.at[0], halos.at[0], sizes, halo_send.at[0], halo_recv.at[0], "wait")
    add_halo(first, halos.at[0])

    l_weights.wait()
    for copy in answers:
        copy.wait_recv()
    for p in range(count):
        masked[p] = arrived[lax.rem(p - s + count, count)] * live_rows(counts, p, capacity)
    forcing[...] = jnp.zeros(forcing.shape, F32)

    def spread_corner(j, carry):
        weight = weights[0, 0, j]
        high, low = [], []
        for p in range(count):
            columns = col_hot[j, :, p * capacity : (p + 1) * capacity]
            for into, part in zip((high, low), split(KAPPA * weight[p : p + 1, :] * masked[p], 2)):
                into.append(scaled_columns(columns, part))
        left = row_hot[j]
        both = nt(left, jnp.concatenate(high, axis=1)) + nt(left, jnp.concatenate(low, axis=1))
        forcing[...] += both
        return carry

    lax.fori_loop(0, cells.shape[2], spread_corner, 0)
    for c in range(3):
        first[c] += TAU * forcing[:, c * span : (c + 1) * span].reshape(depth, width, span)
    take_edges(first, (), edges.at[1])
    halo_copies(edges.at[1], halos.at[1], sizes, halo_send.at[1], halo_recv.at[1], "start")
    blank_ends(halos.at[1], sizes)
    sweep(first, (), forcing, coupling, second)

    l_vhist.wait()
    hist = vhist.shape[1]
    lane = iota((hist, LANES), 1)
    early = jnp.zeros((hist, LANES), F32)
    for h in range(hist):
        product = vhist[0] * vhist[0, h : h + 1, :]
        for c in range(1, 3):
            product = product + vhist[c] * vhist[c, h : h + 1, :]
        early = early + jnp.where(lane == h, jnp.sum(product, axis=1, keepdims=True), 0.0)

    halo_copies(edges.at[1], halos.at[1], sizes, halo_send.at[1], halo_recv.at[1], "wait")
    add_halo(second, halos.at[1])
    fluid = g < groups - 1

    @pl.when(fluid)
    def _():
        fluid_o[0] = second[...]

    @pl.when(jnp.logical_not(fluid))
    def _():
        fluid_o[...] = state[...]

    for c in range(3):
        for t, part in enumerate(split(second[c].reshape(row_count, span).T, 2)):
            sampler[c * span : (c + 1) * span, t * row_count : (t + 1) * row_count] = part
    force[...] = jnp.zeros(force.shape, F32)

    def sample_corner(j, carry):
        cell = cells[0, 0, j]
        weight = weights[0, 0, j]
        here = row_hot[j]
        got = jnp.dot(sampler[...], jnp.concatenate([here, here], axis=0), preferred_element_type=F32)
        for p in range(count):
            mask = iota((span, capacity), 0) == (cell[p : p + 1, :] & (span - 1))
            for c in range(3):
                part = jnp.where(mask, got[c * span : (c + 1) * span, p * capacity : (p + 1) * capacity], 0.0)
                value = jnp.sum(part, axis=0, keepdims=True) * weight[p : p + 1, :]
                force[p, c : c + 1, :] += value
        return carry

    lax.fori_loop(0, cells.shape[2], sample_corner, 0)
    for p in range(count):
        force[p] = force[p] * live_rows(counts, p, capacity)
    pushed = [to_dev(2, force.at[lax.rem(s + b, count)], forces, b, b) for b in range(1, count)]
    for copy in pushed:
        copy.start()
    forces[0] = force[s]

    wide = n_local // ELEM // LANES
    for copy in pushed:
        copy.wait_recv()
    left, high, low = [], [], []
    for b in range(count):
        node = table[b]
        block = node >> elem_shift
        left.append(hot(wide * ELEM, (block >> lane_shift) * ELEM + (node & (ELEM - 1))))
        mask = iota((LANES, capacity), 0) == (block & (LANES - 1))
        for into, part in zip((high, low), split(forces[b], 2)):
            into.append(spread_right(mask, part))
    left = jnp.concatenate(left, axis=1)
    sums[0] = nt(left, jnp.concatenate(high, axis=1)) + nt(left, jnp.concatenate(low, axis=1))
    shared = [
        send(sums.at[0], sums.at[a], group_send.at[a], group_recv.at[a], shifted(me, (a, 0), sizes))
        for a in range(1, groups)
    ]
    for copy in shared:
        copy.start()
    l_flex.wait()
    l_rprev.wait()
    l_sprev.wait()
    l_whist.wait()
    for copy in shared:
        copy.wait_recv()
    total = sums[lax.rem(g + groups, groups)]
    for gs in range(1, groups):
        total = total + sums[lax.rem(g - gs + groups, groups)]
    u = jnp.concatenate(
        [
            jnp.concatenate(
                [total[h * ELEM : (h + 1) * ELEM, c * LANES : (c + 1) * LANES] for h in range(wide)], axis=1
            )
            for c in range(3)
        ],
        axis=0,
    )
    for o in range(3 * ELEM):
        nodal[o : o + 1, :] = jnp.sum(flex[o] * u, axis=0, keepdims=True)

    per_row = LANES // ELEM
    own = iota((ELEM, LANES), 0) == (iota((ELEM, LANES), 1) >> log2(per_row))
    lines = []
    for c in range(3):
        for h in range(wide):
            lines.append(
                jnp.concatenate(
                    [
                        jnp.where(own, nodal[c * ELEM + i : c * ELEM + i + 1, h * LANES : (h + 1) * LANES], 0.0)
                        for i in range(ELEM)
                    ],
                    axis=1,
                )
            )
    lines = jnp.concatenate(lines, axis=0)
    k = iota((ELEM * LANES, LANES), 0)
    move = (k & (per_row - 1)) * ELEM + (k >> lane_shift)
    move = jnp.where(move == iota((ELEM * LANES, LANES), 1), 1.0, 0.0).astype(BF16)
    spread = 0.0
    for part in reversed(split(lines, 3)):
        spread = spread + jnp.dot(part, move, preferred_element_type=F32)
    for c in range(3):
        for h in range(highs):
            solid_s[c : c + 1, h * LANES : (h + 1) * LANES] = spread[c * highs + h : c * highs + h + 1, :]

    order = hist + 1
    solid = solid_s[...]
    residual = solid - disp[...]
    change = residual - rprev[...]
    with_change = vhist[0] * change[0:1, :]
    with_residual = vhist[0] * residual[0:1, :]
    for c in range(1, 3):
        with_change = with_change + vhist[c] * change[c : c + 1, :]
        with_residual = with_residual + vhist[c] * residual[c : c + 1, :]
    cross = jnp.sum(with_change, axis=1, keepdims=True)
    early = early + jnp.where(lane == hist, cross, 0.0)
    early = early + jnp.where(lane == order, jnp.sum(with_residual, axis=1, keepdims=True), 0.0)
    last = jnp.sum(jnp.where(lane == iota((hist, LANES), 0), cross, 0.0), axis=0, keepdims=True)
    lane_one = iota((1, LANES), 1)
    own_square = jnp.sum(jnp.sum(change * change, axis=0, keepdims=True), axis=1, keepdims=True)
    own_right = jnp.sum(jnp.sum(change * residual, axis=0, keepdims=True), axis=1, keepdims=True)
    last = last + jnp.where(lane_one == hist, own_square, 0.0) + jnp.where(lane_one == order, own_right, 0.0)
    grams[0, 0:hist, :] = early
    grams[0, hist : hist + 1, :] = last
    shares = [to_dev(3, grams.at[0], grams, b, b) for b in range(1, count)]
    for copy in shares:
        copy.start()
    image = solid - sprev[...]
    for copy in shares:
        copy.wait_recv()
    m = jnp.zeros((order, LANES), F32)
    for owner in range(count):
        m = m + grams[lax.rem(s - owner + count, count)]
    sub = iota(m.shape, 0)
    for k in range(order):
        row = m[k : k + 1, :] / m[k : k + 1, k : k + 1]
        m = jnp.where(sub == k, row, m - m[:, k : k + 1] * row)
    answer = m[:, order : order + 1]
    for c in range(3):
        old = jnp.sum(answer[0:hist, :] * whist[c], axis=0, keepdims=True)
        result[c : c + 1, :] = solid[c : c + 1, :] - answer[hist : hist + 1, :] * image[c : c + 1, :] - old
    for copy in asked + answers + pushed + shared + shares:
        copy.wait_send()


def store_kernel(fluid_v, result_v, fluid_h, result_h, sems):
    copies = [
        pltpu.make_async_copy(fluid_v, fluid_h, sems.at[0]), pltpu.make_async_copy(result_v, result_h, sems.at[1]),
    ]
    for copy in copies:
        copy.start()
    for copy in copies:
        copy.wait()


def per_device(
    sizes, fluid_state, coupling, displacement, slot_cells, slot_weights, slot_nodes, slot_counts,
    flexibility, resid_prev, struct_prev, v_hist, w_hist,
):
    groups, count = sizes
    comps, depth, width, span = fluid_state.shape[1:]
    capacity = slot_nodes.shape[-1]
    n_local = displacement.shape[1]
    order = v_hist.shape[0] + 1
    dma = pltpu.SemaphoreType.DMA
    vmem = pltpu.VMEM
    args = (
        fluid_state, coupling, displacement, slot_cells, slot_weights, slot_nodes, slot_counts, flexibility,
        resid_prev, struct_prev, v_hist.transpose(1, 0, 2), w_hist.transpose(1, 0, 2),
    )
    small = (1, 6)
    places = [(pltpu.SMEM if k in small else vmem)(a.shape, a.dtype) for k, a in enumerate(args)]
    hbm = pl.BlockSpec(memory_space=pltpu.HBM)
    halo = (2, 2, comps, depth, 1, span)
    slots = (count, 3, capacity)
    shapes = (jax.ShapeDtypeStruct(fluid_state.shape, F32), jax.ShapeDtypeStruct(displacement.shape, F32))
    local = pl.BlockSpec(memory_space=vmem)
    corners = slot_cells.shape[2]
    found = pl.pallas_call(
        functools.partial(kernel, sizes),
        out_shape=shapes,
        in_specs=[hbm] * len(args),
        out_specs=(local, local),
        scratch_shapes=places
        + [
            dma((len(args),)), dma((4, count)), dma((4, count)), dma((groups,)), dma((groups,)),
            dma((2, 2)), dma((2, 2)),
            vmem((count, 1, capacity), jnp.int32), vmem((count, 1, capacity), jnp.int32),
            vmem(halo, F32), vmem(halo, F32),
            vmem((3 * n_local // LANES, LANES), F32), vmem(slots, F32), vmem(slots, F32), vmem(slots, F32),
            vmem((depth * width, 3 * span), F32),
            vmem((comps, depth, width, span), F32), vmem((comps, depth, width, span), F32),
            vmem((3 * span, 2 * depth * width), BF16),
            vmem((corners, depth * width, count * capacity), BF16), vmem((corners, span, count * capacity), BF16),
            vmem(slots, F32), vmem(slots, F32), vmem((groups, n_local // LANES, 3 * LANES), F32),
            vmem((3 * ELEM, n_local // ELEM), F32), vmem((3, n_local), F32), vmem((count, order, LANES), F32),
        ],
        compiler_params=pltpu.CompilerParams(
            collective_id=0, has_side_effects=True, vmem_limit_bytes=56 * 1024 * 1024
        ),
    )(*args)
    return pl.pallas_call(
        store_kernel, out_shape=shapes, in_specs=[local, local], out_specs=(hbm, hbm), scratch_shapes=[dma((2,))]
    )(*found)


def solution(mesh):
    sizes = (mesh.shape["group"], mesh.shape["dev"])
    return jax.shard_map(
        functools.partial(per_device, sizes),
        mesh=mesh,
        in_specs=(
            P("group", None, None, "dev", None),
            P(),
            P(None, "dev"),
            P("group", "dev", None, None, None),
            P("group", "dev", None, None, None),
            P("group", "dev", None, None),
            P("group", "dev", None),
            P(None, None, "dev"),
            P(None, "dev"),
            P(None, "dev"),
            P(None, None, "dev"),
            P(None, None, "dev"),
        ),
        out_specs=(P("group", None, None, "dev", None), P(None, "dev")),
        check_vma=False,
    )
```
